256 devices in a mesh: blk: 64 (over y_hi, x, z), grp: 4 (over y_lo, core).
Axes of the slice: x: 4, y: 4 (y_hi: 2, y_lo: 2; y = y_hi * 2 + y_lo), z: 8, core: 2. Of those that a mesh axis runs over, the one named last changes fastest.
Arguments:
- queries: float32 [32768, 256], P(('blk', 'grp')), may hold values from -20 to 20
- queue: float32 [131072, 256], P(('blk', 'grp')), may hold values from -16 to 16
- new_keys: float32 [32768, 256], P(('blk', 'grp')), may hold values from -3.6 to 3.6
- pos_index: int32 [32768], P(('blk', 'grp')), may hold values from 0 to 32767, as said below
- pointer: int32 [1], replicated, may hold values from 0 to 3
Outputs:
- losses: float32 [32768], P(('blk', 'grp'))
- queue_next: float32 [131072, 256], P(('blk', 'grp'))
The draws below stay inside these ranges and needn't reach their ends.
Inputs may be any that keep to these rules, and one draw needn't show every extreme that they name: pos_index of a query lies in the same aligned block of 128 rows as the query itself, and within each block every row is named exactly once.
All inputs are finite; a program needn't handle non-finite values.
Results may differ from the reference program's by a relative error of at most 0.0012.
Values may be sent and summed in bfloat16 or wider, within the bound.
No kernel may reach another device: no remote copies, remote signals or barrier semaphores. Data moves between devices by JAX's collectives and lax.ppermute only.
A program may use at most 64 MiB of HBM per device.

```python
import math
import jax
import jax.numpy as jnp
from jax import lax

DIM = 256
Q_DEV = 128
SLICE = 512
QTOT = 32768
QUEUE = 131072
N_BLK = 64
N_GRP = 4


def shared_pair(key):
    query_key = jax.random.fold_in(key, 11)
    queue_key = jax.random.fold_in(key, 12)
    queries = jax.random.normal(query_key, (QTOT, DIM), jnp.float32)
    queue = jnp.clip(0.6 * jax.random.normal(queue_key, (QUEUE, DIM), jnp.float32), -3.6, 3.6)
    return (queries, queue)


def draw_queries(key, part):
    return shared_pair(key)[0].astype(jnp.float32)


def draw_queue(key, part):
    return shared_pair(key)[1].astype(jnp.float32)


def draw_pos_index(key, part):
    block_count = QTOT // Q_DEV
    raw_scores = jax.random.randint(jax.random.fold_in(key, 21), (block_count, Q_DEV), 0, 1 << 20)
    distinct = raw_scores * Q_DEV + jnp.arange(Q_DEV, dtype=jnp.int32)[None, :]
    order = jnp.argsort(distinct, axis=1, stable=True).astype(jnp.int32)
    bases = (jnp.arange(block_count, dtype=jnp.int32) * Q_DEV)[:, None]
    return (order + bases).reshape(QTOT).astype(jnp.int32)


def level_of(rng, dims, shards, smallest, top_value):
    gain = 1.0
    for position, blocks in shards:
        draws = jax.random.uniform(jax.random.fold_in(jax.random.fold_in(rng, 6), position), (blocks,), jnp.float32, smallest / len(shards), top_value / len(shards))
        gain = gain * jnp.repeat(jnp.exp(draws), dims[position] // blocks).reshape((-1,) + (1,) * (len(dims) - 1 - position))
    return gain


def noise(key, extent, width, most, split=(), held_as=jnp.bfloat16):
    array = width * jax.random.normal(key, extent, jnp.float32)
    if split:
        array = array * level_of(key, extent, split, -0.22, 0.18)
    return jnp.clip(array, -most, most).astype(held_as)


def setup_inputs(seed: int = 0) -> dict:
    streams_of = jax.random.split(jax.random.key(seed), 6)
    queries = draw_queries(jax.random.fold_in(streams_of[5], 71), 0)
    queue = draw_queue(jax.random.fold_in(streams_of[5], 71), 0)
    new_keys = noise(streams_of[2], (QTOT, DIM), 0.6, 3.6, ((0, 256),), jnp.float32)
    pos_index = draw_pos_index(jax.random.fold_in(streams_of[5], 71), 0)
    pointer = jax.random.randint(streams_of[4], (1,), 0, SLICE // Q_DEV).astype(jnp.int32)
    return {"queries": queries, "queue": queue, "new_keys": new_keys, "pos_index": pos_index, "pointer": pointer}


logit_scale = 5.0
epsilon = 1e-06

def normalize(rows):
    return rows / jnp.sqrt(lax.optimization_barrier(jnp.sum(rows * rows, axis=1, keepdims=True)) + epsilon)

def reference(queries, queue, new_keys, pos_index, pointer):
    qhat = normalize(queries).astype(jnp.bfloat16)
    keys = queue.astype(jnp.bfloat16)
    positives = jnp.take(new_keys.astype(jnp.bfloat16), pos_index, axis=0)
    pos = logit_scale * lax.optimization_barrier(jnp.sum(qhat.astype(jnp.float32) * positives.astype(jnp.float32), axis=1))
    block_rows = math.gcd(QTOT, 64)
    blocks = qhat.reshape(QTOT // block_rows, block_rows, DIM)

    def score_block(query_block):
        scores = logit_scale * jnp.dot(query_block, keys.T, preferred_element_type=jnp.float32)
        top = lax.optimization_barrier(jnp.max(scores, axis=1))
        total = lax.optimization_barrier(jnp.sum(jnp.exp(scores - top[:, None]), axis=1))
        return (top, total)
    top, total = lax.map(score_block, blocks)
    top = top.reshape(QTOT)
    total = total.reshape(QTOT)
    high = jnp.maximum(top, pos)
    losses = high + jnp.log(jnp.exp(pos - high) + total * jnp.exp(top - high)) - pos
    devices_all = N_BLK * N_GRP
    blocks_queue = queue.reshape(devices_all, SLICE, DIM)
    incoming = jnp.roll(new_keys.reshape(devices_all, Q_DEV, DIM), 1, axis=0)
    start = (pointer[0] * Q_DEV).astype(jnp.int32)
    updated = lax.dynamic_update_slice(blocks_queue, incoming, (jnp.int32(0), start, jnp.int32(0)))
    return (losses, updated.reshape(QUEUE, DIM))
```

```python
import math

import jax
import jax.numpy as jnp
from jax import lax
from jax.experimental import pallas as pl
from jax.experimental.pallas import tpu as pltpu
from jax.sharding import Mesh
from jax.sharding import PartitionSpec as P

AXES = ("yh", "x", "z", "yl", "c")
XY = ("yh", "x", "yl")

logit_scale = 5.0
epsilon = 1e-06
SCALE2 = logit_scale / math.log(2.0)
LN2 = math.log(2.0)
LOWEST = -1e30


def shifted(value, axis, steps):
    count = lax.axis_size(axis)
    return lax.ppermute(value, axis, [(k, (k + steps) % count) for k in range(count)])


def to_everyone(x, axis):
    count = lax.axis_size(axis)
    return lax.all_to_all(jnp.broadcast_to(x[None], (count, *x.shape)), axis, 0, 0, tiled=True)


def normalize(rows):
    return rows / jnp.sqrt(jnp.sum(rows * rows, axis=1, keepdims=True) + epsilon)


def fold_kernel(*refs, n_q, n_k):
    q_refs, k_refs = refs[:n_q], refs[n_q : n_q + n_k]
    m_in, l_in, m_out, l_out = refs[n_q + n_k :]
    for a in range(n_q):
        query = q_refs[a][...]
        top, total = m_in[a], l_in[a]
        for k_ref in k_refs:
            scores = lax.dot_general(
                k_ref[...], query, (((1,), (1,)), ((), ())), preferred_element_type=jnp.float32
            )
            scores = scores.reshape(-1, 8, scores.shape[1])
            new_top = jnp.maximum(top, jnp.max(scores, axis=0))
            weight = jnp.exp2((scores - new_top[None]) * SCALE2)
            total = total * jnp.exp2((top - new_top) * SCALE2) + jnp.sum(weight, axis=0)
            top = new_top
        m_out[a], l_out[a] = top, total


def fold(queries, keys, state, width=256):
    n_q, n_k, rows, dim = len(queries), len(keys), queries[0].shape[0], queries[0].shape[1]
    state_spec = pl.BlockSpec((n_q, 8, width), lambda i: (0, 0, i))
    shape = jax.ShapeDtypeStruct((n_q, 8, rows), jnp.float32)
    n_keys = sum(k.shape[0] for k in keys)
    return pl.pallas_call(
        lambda *refs: fold_kernel(*refs, n_q=n_q, n_k=n_k),
        name="fold",
        grid=(rows // width,),
        in_specs=[pl.BlockSpec((width, dim), lambda i: (i, 0))] * n_q
        + [pl.BlockSpec(k.shape, lambda i: (0, 0)) for k in keys]
        + [state_spec, state_spec],
        out_specs=[state_spec, state_spec],
        out_shape=[shape, shape],
        cost_estimate=pl.CostEstimate(
            flops=2 * n_q * rows * n_keys * dim,
            transcendentals=n_q * rows * n_keys,
            bytes_accessed=2 * dim * (n_q * rows + n_keys),
        ),
    )(*queries, *keys, *state)


def per_device(queries, queue, new_keys, pos_index, pointer):
    count = queries.shape[0]
    keys = queue.astype(jnp.bfloat16)
    n_z = lax.axis_size("z")
    forward, backward = shifted(keys, "z", 1), shifted(keys, "z", -1)

    qhat = normalize(queries).astype(jnp.bfloat16)
    group = to_everyone(qhat, XY).reshape(-1, qhat.shape[1])
    other = shifted(group, "c", 1)
    pair = (group, other)
    shape = (2, 8, group.shape[0])
    state = (jnp.full(shape, LOWEST, jnp.float32), jnp.zeros(shape, jnp.float32))

    arrived = (keys,)
    for step in range(1, n_z // 2):
        if step < n_z // 2 - 1:
            next_forward, next_backward = shifted(forward, "z", 1), shifted(backward, "z", -1)
        else:
            half = keys.shape[0] // 2
            next_forward = shifted(forward[:half], "z", 1)
            next_backward = shifted(backward[half:], "z", -1)
        state = fold(pair, arrived, state)
        arrived = (forward, backward)
        forward, backward = next_forward, next_backward
    state = fold(pair, arrived, state)
    state = fold(pair, (forward, backward), state)

    top, total = state
    top_all = jnp.max(top, axis=1)
    total_all = jnp.sum(total * jnp.exp2((top - top_all[:, None]) * SCALE2), axis=1)
    lse = top_all * logit_scale + jnp.log(total_all)
    theirs = shifted(lse[1], "c", 1)
    mine = jnp.logaddexp(lse[0], theirs).reshape(-1, 1, count)
    found = lax.all_to_all(mine, XY, 0, 0, tiled=True).reshape(-1, count)
    top = jnp.max(found, axis=0)
    total = jnp.sum(jnp.exp(found - top[None]), axis=0)

    rank = lax.axis_index(AXES)
    positives = jnp.take(new_keys.astype(jnp.bfloat16), pos_index - rank * count, axis=0)
    pos = logit_scale * jnp.sum(qhat.astype(jnp.float32) * positives.astype(jnp.float32), axis=1)
    high = jnp.maximum(top, pos)
    losses = high + jnp.log(jnp.exp(pos - high) + total * jnp.exp(top - high)) - pos

    incoming = shifted(new_keys, AXES, 1)
    start = pointer[0] * count
    queue_next = lax.dynamic_update_slice(queue, incoming, (start, jnp.int32(0)))
    return (losses, queue_next)


def solution(mesh):
    finer = Mesh(mesh.devices.reshape(2, 4, 8, 2, 2), AXES)
    return jax.shard_map(
        per_device,
        mesh=finer,
        in_specs=(P(AXES, None), P(AXES, None), P(AXES, None), P(AXES), P()),
        out_specs=(P(AXES), P(AXES, None)),
        check_vma=False,
    )
```
